32 devices in a mesh: member: 2 (over y), lat: 4 (over z), lon: 2 (over x), lev: 2 (over core).
Axes of the slice: x: 2, y: 2, z: 4, core: 2. Of those that a mesh axis runs over, the one named last changes fastest.
Arguments:
- perturbation: bfloat16 [4, 64, 16, 8, 128], P('member', 'lev', 'lat', 'lon'), parts along dimension 0, may hold values from -6 to 6
- adjoint_forcing: bfloat16 [4, 64, 16, 8, 128], P('member', 'lev', 'lat', 'lon'), parts along dimension 0, may hold values from -6 to 6
- source_rows: int32 [16, 8, 4], P('lat', 'lon'), may hold values from 0 to 15, as said below
- source_cols: int32 [16, 8, 4], P('lat', 'lon'), may hold values from 0 to 7, as said below
- cubic_weights: bfloat16 [16, 8, 4, 128, 128], P('lat', 'lon'), may hold values from -1.5 to 1.5
Outputs:
- tangent_out: bfloat16 [4, 64, 16, 8, 128], P('member', 'lev', 'lat', 'lon'), parts along dimension 0
- adjoint_out: bfloat16 [4, 64, 16, 8, 128], P('member', 'lev', 'lat', 'lon'), parts along dimension 0
The draws below stay inside these ranges and needn't reach their ends.
There are 2 independent parts, one for each index of `member`. The reference program is written for one: setup_inputs(seed, part) draws one part's arguments, and reference() takes and returns one part's arrays. A program takes and returns all parts, laid end to end along the dimension named above; an argument that names none is the same for every part. Nothing has to cross between parts.
Inputs may be any that keep to these rules, and one draw needn't show every extreme that they name: source_rows[i, j, k] differs from i by at most 8. source_cols[i, j, k] is j + d modulo 8 with d from -1 to 1, and from -2 to 2 where i lies in the first or last 4 block rows.
All inputs are finite; a program needn't handle non-finite values.
Results may differ from the reference program's by a relative error of at most 0.004.
Values may be sent and summed in bfloat16 or wider, within the bound.
A program may use at most 64 MiB of HBM per device.

```python
import math
import jax
import jax.numpy as jnp
from jax import lax

CELLS = 128
STENCIL = 4
BAND_ROWS = 4
FIELDS = 2
LEVELS = 64
LAT_ROWS = 16
LON_COLS = 8
N_LAT = 4


def draw_source_rows(key, part):
    first_key, second_key = jax.random.split(jax.random.fold_in(key, 11))
    row_ids = jnp.arange(LAT_ROWS, dtype=jnp.int32)[:, None, None]
    reach_rows = 2 * BAND_ROWS
    shape = (LAT_ROWS, LON_COLS, STENCIL)
    offsets = jax.random.randint(first_key, shape, -reach_rows, reach_rows + 1)
    signs = 2 * jax.random.randint(second_key, shape, 0, 2) - 1
    last_one = jnp.arange(STENCIL, dtype=jnp.int32)[None, None, :] == STENCIL - 1
    offsets = jnp.where(last_one, signs * reach_rows, offsets)
    return jnp.clip(row_ids + offsets, 0, LAT_ROWS - 1).astype(jnp.int32)


def draw_source_cols(key, part):
    first_key, second_key = jax.random.split(jax.random.fold_in(key, 23))
    row_ids = jnp.arange(LAT_ROWS, dtype=jnp.int32)[:, None, None]
    band_ids = row_ids // BAND_ROWS
    polar = (band_ids == 0) | (band_ids == N_LAT - 1)
    reach_cols = jnp.where(polar, 2, 1)
    col_ids = jnp.arange(LON_COLS, dtype=jnp.int32)[None, :, None]
    shape = (LAT_ROWS, LON_COLS, STENCIL)
    offsets = jax.random.randint(first_key, shape, -2, 3)
    offsets = jnp.clip(offsets, -reach_cols, reach_cols)
    signs = 2 * jax.random.randint(second_key, shape, 0, 2) - 1
    last_one = jnp.arange(STENCIL, dtype=jnp.int32)[None, None, :] == STENCIL - 1
    offsets = jnp.where(last_one & polar, signs * 2, offsets)
    return jnp.mod(col_ids + offsets, LON_COLS).astype(jnp.int32)


def draw_cubic_weights(key, part):
    second_key = jax.random.fold_in(jax.random.fold_in(key, 37), 1)
    identity = jnp.eye(CELLS, dtype=jnp.float32)
    diagonal = jnp.full((LAT_ROWS, LON_COLS, STENCIL, 1, 1), 0.5, jnp.float32)
    noise = jax.random.normal(second_key, (LAT_ROWS, LON_COLS, STENCIL, CELLS, CELLS), jnp.float32)
    noise = jnp.clip(noise * (0.35 / math.sqrt(CELLS)), -0.6, 0.6)
    return (diagonal * identity + noise).astype(jnp.bfloat16)


def steps_of(rng, shape, shards, least, largest):
    loudness, own = 1.0, jax.random.fold_in(rng, 6)
    for axis_at, blocks in shards:
        draws = jnp.exp(jax.random.uniform(jax.random.fold_in(own, axis_at), (blocks,), jnp.float32, least / len(shards), largest / len(shards)))
        loudness = loudness * jnp.repeat(draws, shape[axis_at] // blocks).reshape([-1 if axis == axis_at else 1 for axis in range(len(shape))])
    return loudness


def centred(key, shape, scale, reach, cuts=(), kind=jnp.bfloat16):
    drawn = scale * jax.random.normal(key, shape, jnp.float32)
    if cuts:
        drawn = drawn * steps_of(key, shape, cuts, -0.22, 0.18)
    return jnp.clip(drawn, -reach, reach).astype(kind)


def setup_inputs(seed: int = 0, part: int = 0) -> dict:
    arg_keys = jax.random.split(jax.random.key(seed), 6)
    part_splits = jax.random.split(jax.random.fold_in(arg_keys[5], part), 6)
    return {
        "perturbation": centred(part_splits[0], (FIELDS, LEVELS, LAT_ROWS, LON_COLS, CELLS), 1.0, 6.0, ((1, 2), (2, 4), (3, 2))),
        "adjoint_forcing": centred(part_splits[1], (FIELDS, LEVELS, LAT_ROWS, LON_COLS, CELLS), 1.0, 6.0, ((1, 2), (2, 4), (3, 2))),
        "source_rows": draw_source_rows(jax.random.fold_in(arg_keys[5], 71), part),
        "source_cols": draw_source_cols(jax.random.fold_in(arg_keys[5], 71), part),
        "cubic_weights": draw_cubic_weights(jax.random.fold_in(arg_keys[5], 71), part),
    }


def interpolate(field, source_rows, source_cols, cubic_weights):

    def one_row(pieces):
        rows_here, cols_here, weights_here = pieces
        picked = field[:, :, rows_here, cols_here, :]
        return jnp.einsum('flnks,nksc->flnc', picked, weights_here.astype(jnp.float32), precision=lax.Precision.HIGHEST)
    mapped = lax.map(one_row, (source_rows, source_cols, cubic_weights))
    return jnp.transpose(mapped, (1, 2, 0, 3, 4))

def reference(perturbation, adjoint_forcing, source_rows, source_cols, cubic_weights):

    def linear_map(field):
        return interpolate(field, source_rows, source_cols, cubic_weights)
    tangent, pullback = jax.vjp(linear_map, perturbation.astype(jnp.float32))
    adjoint = pullback(adjoint_forcing.astype(jnp.float32))[0]
    return (tangent.astype(jnp.bfloat16), adjoint.astype(jnp.bfloat16))
```

```python
import functools
import jax
import jax.numpy as jnp
from jax import lax
from jax.experimental import pallas as pl
from jax.experimental.pallas import tpu as pltpu
from jax.sharding import PartitionSpec as P

REACH = 2
HALO = 2
BANDS = 2 * REACH + 1
PAD = 8
STEPS = (1, -1)
MESH = pl.DeviceIdType.MESH
BF16, F32 = jnp.bfloat16, jnp.float32


def exchange(
    sizes,
    rows_ref, cols_ref, own_hbm, forcing_hbm, weights_hbm,
    tangent_ref, adjoint_ref,
    raw, forcing, weights, ext, picked, turned, spread, gather,
    ax_out, ax_in, far_out, far_in, near_out, near_in, lent,
    load_sem, zf_send, zf_recv, xf_send, xf_recv, ax_send, ax_recv, az_send, az_recv,
    fwd_send, fwd_recv, lend_send, lend_recv,
):
    lat_count, lon_count, rows, cols, stencil = sizes
    depth, tile, cells = raw.shape
    pair = 2 * rows
    sides = 1 if lon_count == 2 else 2
    group = tile + sides * tile
    places = BANDS * group
    picks = tile * stencil
    pitch = depth + PAD
    total_cols = cols * lon_count
    lat_rows = (2 * REACH + 1) * rows
    z = lax.axis_index("lat")
    x = lax.axis_index("lon")
    east = lax.rem(x + 1, lon_count)
    west = lax.rem(x + lon_count - 1, lon_count)
    out_side = (east, west)[:sides]
    back = (0,) if sides == 1 else (1, 0)
    last = lat_count - 1
    polar = (z == 0) | (z == last)
    inland = jnp.logical_not(polar)
    poles = ((0, 1), (last, -1))
    kinds = (0, 1)

    def there(offset):
        return (z + offset >= 0) & (z + offset < lat_count)

    def slot(band, kind, side=None):
        first = (band + REACH) * group + kind * pair
        if side is not None:
            first += tile * (1 + side)
        return pl.ds(first, pair)

    def when(condition, act):
        pl.when(condition)(act)

    def loads():
        return (
            pltpu.make_async_copy(own_hbm, raw, load_sem.at[0]),
            pltpu.make_async_copy(forcing_hbm, forcing, load_sem.at[1]),
            pltpu.make_async_copy(weights_hbm, weights, load_sem.at[2]),
        )

    barrier = pltpu.get_barrier_semaphore()
    for side in out_side:
        pl.semaphore_signal(barrier, inc=1, device_id={"lon": side}, device_id_type=MESH)
    for step in STEPS:
        @pl.when(there(step))
        def _():
            pl.semaphore_signal(barrier, inc=1, device_id={"lat": z + step}, device_id_type=MESH)
    for copy in loads():
        copy.start()

    def zf(d, hop, kind):
        band = -STEPS[d] * hop
        return pltpu.make_async_remote_copy(
            src_ref=ext.at[:, slot(band, kind), :],
            dst_ref=ext.at[:, slot(band - STEPS[d], kind), :],
            send_sem=zf_send.at[d, hop, kind],
            recv_sem=zf_recv.at[d, hop, kind],
            device_id={"lat": z + STEPS[d]},
            device_id_type=MESH,
        )

    def xf(band, kind, side):
        return pltpu.make_async_remote_copy(
            src_ref=ext.at[:, slot(band, kind), :],
            dst_ref=ext.at[:, slot(band, kind, back[side]), :],
            send_sem=xf_send.at[band + REACH, kind, side],
            recv_sem=xf_recv.at[band + REACH, kind, back[side]],
            device_id={"lon": out_side[side]},
            device_id_type=MESH,
        )

    def xf_in(band, kind, side):
        return pltpu.make_async_remote_copy(
            src_ref=ext.at[:, slot(band, kind), :],
            dst_ref=ext.at[:, slot(band, kind, side), :],
            send_sem=xf_send.at[band + REACH, kind, side],
            recv_sem=xf_recv.at[band + REACH, kind, side],
            device_id={"lon": out_side[side]},
            device_id_type=MESH,
        )

    def ax(band, kind, side, arrive=False):
        land = side if arrive else back[side]
        return pltpu.make_async_remote_copy(
            src_ref=ax_out.at[band + REACH, side, kind],
            dst_ref=ax_in.at[band + REACH, land, kind],
            send_sem=ax_send.at[band + REACH, kind, side],
            recv_sem=ax_recv.at[band + REACH, kind, land],
            device_id={"lon": out_side[side]},
            device_id_type=MESH,
        )

    def az(d, near, kind):
        return pltpu.make_async_remote_copy(
            src_ref=(near_out if near else far_out).at[d, kind],
            dst_ref=(near_in if near else far_in).at[d, kind],
            send_sem=az_send.at[d, near, kind],
            recv_sem=az_recv.at[d, near, kind],
            device_id={"lat": z + STEPS[d]},
            device_id_type=MESH,
        )

    def fwd(pole, step, i, side):
        return pltpu.make_async_remote_copy(
            src_ref=ext.at[:, slot(i * step, 0, side), :],
            dst_ref=ext.at[:, slot((i + 1) * step, 0, side), :],
            send_sem=fwd_send.at[i, side],
            recv_sem=fwd_recv.at[i, side],
            device_id={"lat": pole},
            device_id_type=MESH,
        )

    def lend(pole, step, i, side):
        return pltpu.make_async_remote_copy(
            src_ref=ax_out.at[(i + 1) * step + REACH, side, 0],
            dst_ref=lent.at[i, side],
            send_sem=lend_send.at[i, side],
            recv_sem=lend_recv.at[i, side],
            device_id={"lat": pole + step},
            device_id_type=MESH,
        )

    def x_start(make, band, kind):
        for side in range(sides):
            make(band, kind, side).start()

    span = tile * 8
    to = lax.broadcasted_iota(jnp.int32, (span, span), 0)
    come = lax.broadcasted_iota(jnp.int32, (span, span), 1)

    def column_of(place):
        position = (place % tile) // rows
        return jnp.where(position < 2, position * (cols - 1), position - 1)

    def shuffle(a, b):
        same = (a // tile == b // tile) & (b % tile == (a % rows) * cols + column_of(a))
        return jnp.where(same, 1.0, 0.0).astype(BF16)

    order = shuffle(to, come)
    own = pl.ds(REACH * group, tile)
    loads()[0].wait()
    for i in range(depth // 8):
        block = raw[pl.ds(i * 8, 8)].reshape(span, cells)
        block = jnp.dot(order, block, preferred_element_type=F32).astype(BF16)
        ext[pl.ds(i * 8, 8), own, :] = block.reshape(8, tile, cells)

    greeted = sides + jnp.where(there(1), 1, 0) + jnp.where(there(-1), 1, 0)
    pl.semaphore_wait(barrier, greeted)

    for kind in kinds:
        for d in range(2):
            when(there(STEPS[d]), lambda: zf(d, 0, kind).start())
        if kind == 0:
            x_start(xf, 0, 0)
        else:
            when(polar, lambda: x_start(xf, 0, 1))

    blank = jnp.zeros((depth, tile, cells), BF16)
    for band in range(-REACH, REACH + 1):
        @pl.when(jnp.logical_not(there(band)))
        def _():
            for part in range(group // tile):
                ext[:, pl.ds((band + REACH) * group + part * tile, tile), :] = blank

        @pl.when(there(band) & inland)
        def _():
            for side in range(sides):
                ext[:, slot(band, 1, side), :] = jnp.zeros((depth, pair, cells), BF16)

    lane = lax.broadcasted_iota(jnp.int32, (1, places), 1)
    within = lane % group
    half = within % tile
    position = HALO + jnp.where(half // rows < 2, (half // rows) * (cols - 1), half // rows - 1)
    area = within // tile
    position = position + jnp.where(area == 1, cols, jnp.where(area == 2, -cols, 0))
    position = (position + total_cols) % total_cols
    code = position * lat_rows + (lane // group) * rows + half % rows

    def select(t, carry):
        i, j = t // cols, t % cols
        for k in range(stencil):
            row = rows_ref[i, j, k] - z * rows + REACH * rows
            col = cols_ref[i, j, k] - x * cols + HALO
            col = col + jnp.where(col < 0, total_cols, 0)
            col = col - jnp.where(col >= total_cols, total_cols, 0)
            gather[pl.ds(t * stencil + k, 1), :] = jnp.where(
                code == col * lat_rows + row, 1.0, 0.0
            )
        return carry

    lax.fori_loop(0, tile, select, 0, unroll=2)
    chosen = gather[...]
    scatter = chosen.T.astype(BF16)

    loads()[1].wait()

    def turn(d, carry):
        turned[pl.ds(d, tile, stride=pitch), :] = forcing[d].astype(F32)
        return carry

    lax.fori_loop(0, depth, turn, 0, unroll=8)
    loads()[2].wait()

    def contribute(t, carry):
        block = weights[pl.ds(t * stencil, stencil)].reshape(stencil * cells, cells)
        here = turned[pl.ds(pl.multiple_of(t * pitch, 8), depth), :].astype(BF16)
        part = lax.dot_general(
            here, block, (((1,), (1,)), ((), ())), preferred_element_type=F32
        )
        for k in range(stencil):
            picked[pl.ds(t * stencil + k, depth, stride=picks + PAD), :] = part[
                :, k * cells : (k + 1) * cells
            ]
        return carry

    lax.fori_loop(0, tile, contribute, 0, unroll=2)

    def add_up(i, carry):
        pieces = []
        for e in range(2):
            first = pl.multiple_of((i * 2 + e) * (picks + PAD), 8)
            pieces.append(picked[pl.ds(first, picks), :].astype(BF16))
        summed = jnp.dot(
            scatter, jnp.concatenate(pieces, axis=1), preferred_element_type=F32
        )
        for e in range(2):
            d = i * 2 + e
            value = summed[:, e * cells : (e + 1) * cells]
            for band in range(BANDS):
                first = band * group
                spread[d, pl.ds(band * tile, tile), :] = value[first : first + tile]
                for side in range(sides):
                    first += tile
                    for kind in kinds:
                        ax_out[band, side, kind, d] = value[
                            first + kind * pair : first + (kind + 1) * pair
                        ].astype(BF16)
        return carry

    lax.fori_loop(0, depth // 2, add_up, 0, unroll=2)

    def total(band, kind):
        return spread.at[:, pl.ds((band + REACH) * tile + kind * pair, pair), :]

    def take(band, kind):
        for side in range(sides):
            ax(band, kind, side, True).wait_recv()
            total(band, kind)[...] += ax_in[band + REACH, side, kind].astype(F32)

    def send_far(d, kind):
        far_out[d, kind] = total(2 * STEPS[d], kind)[...].astype(BF16)
        az(d, 0, kind).start()

    def send_near(d, kind):
        @pl.when(there(-STEPS[d]))
        def _():
            az(d, 0, kind).wait_recv()
            total(STEPS[d], kind)[...] += far_in[d, kind].astype(F32)

        near_out[d, kind] = total(STEPS[d], kind)[...].astype(BF16)
        az(d, 1, kind).start()

    def borrow(pole, step, i):
        for side in range(sides):
            lend(pole, step, i, side).wait_recv()
            mine = ax_out.at[i * step + REACH, side, 0]
            mine[...] = (mine[...].astype(F32) + lent[i, side].astype(F32)).astype(BF16)
        x_start(ax, i * step, 0)

    for pole, step in poles:
        @pl.when(z == pole)
        def _():
            x_start(ax, 2 * step, 1)
            for side in range(sides):
                lend(pole, step, 1, side).start()
    for d in range(2):
        when(there(2 * STEPS[d]) & inland, lambda: x_start(ax, 2 * STEPS[d], 0))
    for pole, step in poles:
        when(z == pole, lambda: send_far(STEPS.index(step), 0))
    for d in range(2):
        @pl.when(there(-STEPS[d]))
        def _():
            zf(d, 0, 0).wait_recv()
            when(there(STEPS[d]), lambda: zf(d, 1, 0).start())
    for pole, step in poles:
        @pl.when(z == pole + step)
        def _():
            for side in range(sides):
                xf_in(0, 0, side).wait_recv()
            for side in range(sides):
                fwd(pole, step, 0, side).start()
            x_start(xf, step, 0)
            x_start(ax, -step, 0)
    inner = (z > 1) & (z < last - 1)

    @pl.when(inner)
    def _():
        for step in STEPS:
            x_start(ax, step, 0)
            x_start(xf, step, 0)

    for d in range(2):
        when(there(2 * STEPS[d]) & inland, lambda: send_far(d, 1))
    for d in range(2):
        @pl.when(there(-STEPS[d]))
        def _():
            zf(d, 0, 1).wait_recv()
            when(there(STEPS[d]), lambda: zf(d, 1, 1).start())
    for pole, step in poles:
        @pl.when(z == pole)
        def _():
            x_start(xf, step, 1)
            x_start(ax, step, 1)
            take(2 * step, 1)
            send_far(STEPS.index(step), 1)
            for side in range(sides):
                lend(pole, step, 0, side).start()
            send_near(STEPS.index(step), 0)
    for d in range(2):
        @pl.when(there(2 * STEPS[d]) & inland)
        def _():
            take(2 * STEPS[d], 0)
            send_far(d, 0)
    for pole, step in poles:
        @pl.when(z == pole + step)
        def _():
            borrow(pole, step, 1)
            x_start(xf, -step, 0)
            for side in range(sides):
                xf_in(step, 0, side).wait_recv()
            for side in range(sides):
                fwd(pole, step, 1, side).start()
    for d in range(2):
        @pl.when(there(-2 * STEPS[d]))
        def _():
            zf(d, 1, 0).wait_recv()
            when(inland, lambda: x_start(xf, -2 * STEPS[d], 0))
    for d in range(2):
        @pl.when(there(-2 * STEPS[d]))
        def _():
            zf(d, 1, 1).wait_recv()
            when(polar, lambda: x_start(xf, -2 * STEPS[d], 1))
    when(inner, lambda: x_start(ax, 0, 0))
    for pole, step in poles:
        @pl.when(z == pole)
        def _():
            x_start(ax, 0, 0)
            x_start(ax, 0, 1)
    for pole, step in poles:
        @pl.when(z == pole)
        def _():
            take(step, 1)
            send_near(STEPS.index(step), 1)

        @pl.when(z == pole + step)
        def _():
            send_near(STEPS.index(step), 1)
            take(-step, 0)
            send_near(STEPS.index(-step), 0)
            send_near(STEPS.index(-step), 1)
            take(step, 0)
            send_near(STEPS.index(step), 0)
            borrow(pole, step, 0)

    @pl.when(inner)
    def _():
        for d in range(2):
            send_near(d, 1)
        for d in range(2):
            take(STEPS[d], 0)
            send_near(d, 0)

    for pole, step in poles:
        @pl.when(z == pole)
        def _():
            for side in range(sides):
                for kind in kinds:
                    xf_in(0, kind, side).wait_recv()
                for i in range(2):
                    xf_in((i + 1) * step, 1, side).wait_recv()
                    fwd(pole, step, i, side).wait_recv()

        @pl.when(z == pole + step)
        def _():
            for side in range(sides):
                xf_in(-step, 0, side).wait_recv()

    @pl.when(inner)
    def _():
        for band in range(-1, 2):
            for side in range(sides):
                xf_in(band, 0, side).wait_recv()

    for d in range(2):
        @pl.when(there(2 * STEPS[d]) & inland)
        def _():
            for side in range(sides):
                xf_in(2 * STEPS[d], 0, side).wait_recv()

    chosen = gather[...].astype(BF16)

    def collect(i, carry):
        block = jnp.concatenate([ext[i * 2], ext[i * 2 + 1]], axis=1)
        value = jnp.dot(chosen, block, preferred_element_type=F32)
        for e in range(2):
            picked[pl.ds(i * 2 + e, picks, stride=pitch), :] = value[
                :, e * cells : (e + 1) * cells
            ]
        return carry

    lax.fori_loop(0, depth // 2, collect, 0, unroll=2)

    def interpolate(t, carry):
        sources = []
        for k in range(stencil):
            first = pl.multiple_of((t * stencil + k) * pitch, 8)
            sources.append(picked[pl.ds(first, depth), :].astype(BF16))
        block = weights[pl.ds(t * stencil, stencil)].reshape(stencil * cells, cells)
        value = jnp.dot(
            jnp.concatenate(sources, axis=1), block, preferred_element_type=F32
        )
        tangent_ref[t] = value.astype(BF16)
        return carry

    lax.fori_loop(0, tile, interpolate, 0, unroll=2)

    take(0, 0)
    when(polar, lambda: take(0, 1))
    for d in range(2):
        @pl.when(there(-STEPS[d]))
        def _():
            for kind in kinds:
                az(d, 1, kind).wait_recv()
                total(0, kind)[...] += near_in[d, kind].astype(F32)
    order = shuffle(come, to)
    for i in range(depth // 8):
        block = spread[pl.ds(i * 8, 8), pl.ds(REACH * tile, tile), :].astype(BF16)
        block = jnp.dot(order, block.reshape(span, cells), preferred_element_type=F32)
        adjoint_ref[pl.ds(i * 8, 8)] = block.astype(BF16).reshape(8, tile, cells)

    for d in range(2):
        @pl.when(there(STEPS[d]))
        def _():
            for kind in kinds:
                zf(d, 0, kind).wait_send()
                az(d, 1, kind).wait_send()

                @pl.when(there(-STEPS[d]))
                def _():
                    zf(d, 1, kind).wait_send()

                @pl.when(there(2 * STEPS[d]))
                def _():
                    az(d, 0, kind).wait_send()
    for side in range(sides):
        for make in (xf, ax):
            make(0, 0, side).wait_send()
            for band in range(-REACH, REACH + 1):
                if band != 0:
                    when(there(band) & inland, lambda: make(band, 0, side).wait_send())
                when(there(band) & polar, lambda: make(band, 1, side).wait_send())
        for pole, step in poles:
            for i in range(2):
                when(z == pole, lambda: lend(pole, step, i, side).wait_send())
                when(z == pole + step, lambda: fwd(pole, step, i, side).wait_send())


def on_device(perturbation, adjoint_forcing, source_rows, source_cols, cubic_weights):
    fields, levels, rows, cols, cells = perturbation.shape
    stencil = source_rows.shape[2]
    depth = fields * levels
    tile = rows * cols
    picks = tile * stencil
    lat_count = lax.axis_size("lat")
    lon_count = lax.axis_size("lon")
    assert cols == 2 * HALO and rows >= 4 and lat_count >= 4 and lon_count >= 2
    sides = 1 if lon_count == 2 else 2
    places = BANDS * tile * (1 + sides)
    half = (depth, 2 * rows, cells)
    own = perturbation.reshape(depth, tile, cells)
    forcing = adjoint_forcing.reshape(depth, tile, cells)
    weights = cubic_weights.reshape(picks, cells, cells)

    vmem = pl.BlockSpec(memory_space=pltpu.VMEM)
    hbm = pl.BlockSpec(memory_space=pltpu.HBM)
    smem = pl.BlockSpec(memory_space=pltpu.SMEM)
    dma = pltpu.SemaphoreType.DMA
    tangent, adjoint = pl.pallas_call(
        functools.partial(exchange, (lat_count, lon_count, rows, cols, stencil)),
        name="exchange",
        out_shape=(
            jax.ShapeDtypeStruct((tile, depth, cells), BF16),
            jax.ShapeDtypeStruct((depth, tile, cells), BF16),
        ),
        in_specs=[smem, smem, hbm, hbm, hbm],
        out_specs=(vmem, vmem),
        scratch_shapes=[
            pltpu.VMEM((depth, tile, cells), BF16),
            pltpu.VMEM((depth, tile, cells), BF16),
            pltpu.VMEM((picks, cells, cells), BF16),
            pltpu.VMEM((depth, places, cells), BF16),
            pltpu.VMEM((max(picks, depth) * (max(picks, depth) + PAD), cells), F32),
            pltpu.VMEM((tile * (depth + PAD), cells), F32),
            pltpu.VMEM((depth, BANDS * tile, cells), F32),
            pltpu.VMEM((picks, places), F32),
            pltpu.VMEM((BANDS, sides, 2) + half, BF16),
            pltpu.VMEM((BANDS, sides, 2) + half, BF16),
            pltpu.VMEM((2, 2) + half, BF16),
            pltpu.VMEM((2, 2) + half, BF16),
            pltpu.VMEM((2, 2) + half, BF16),
            pltpu.VMEM((2, 2) + half, BF16),
            pltpu.VMEM((2, sides) + half, BF16),
            dma((3,)),
            dma((2, 2, 2)),
            dma((2, 2, 2)),
            dma((BANDS, 2, sides)),
            dma((BANDS, 2, sides)),
            dma((BANDS, 2, sides)),
            dma((BANDS, 2, sides)),
            dma((2, 2, 2)),
            dma((2, 2, 2)),
            dma((2, sides)),
            dma((2, sides)),
            dma((2, sides)),
            dma((2, sides)),
        ],
        compiler_params=pltpu.CompilerParams(
            collective_id=0, has_side_effects=True, vmem_limit_bytes=56 * 1024 * 1024
        ),
    )(source_rows, source_cols, own, forcing, weights)

    tangent_out = tangent.reshape(rows, cols, fields, levels, cells).transpose(2, 3, 0, 1, 4)
    adjoint_out = adjoint.reshape(fields, levels, rows, cols, cells)
    return (tangent_out, adjoint_out)


def solution(mesh):
    placed = (
        P("member", "lev", "lat", "lon", None),
        P("member", "lev", "lat", "lon", None),
        P("lat", "lon", None),
        P("lat", "lon", None),
        P("lat", "lon", None, None, None),
    )
    return jax.shard_map(
        on_device,
        mesh=mesh,
        in_specs=placed,
        out_specs=(P("member", "lev", "lat", "lon", None), P("member", "lev", "lat", "lon", None)),
        check_vma=False,
    )
```

```python
import functools
import jax
import jax.numpy as jnp
from jax import lax
from jax.experimental import pallas as pl
from jax.experimental.pallas import tpu as pltpu
from jax.sharding import PartitionSpec as P

REACH = 2
HALO = 2
BANDS = 2 * REACH + 1
PAD = 8
STEPS = (1, -1)
MESH = pl.DeviceIdType.MESH
BF16, F32 = jnp.bfloat16, jnp.float32


def exchange(
    sizes,
    rows_hbm, cols_hbm, own_hbm, forcing_hbm, weights_hbm,
    tangent_ref, adjoint_ref,
    rows_ref, cols_ref, raw, forcing, weights, ext, picked, turned, spread, gather,
    ax_out, ax_in, far_out, far_in, near_out, near_in, lent,
    load_sem, zf_send, zf_recv, xf_send, xf_recv, ax_send, ax_recv, az_send, az_recv,
    fwd_send, fwd_recv, lend_send, lend_recv,
):
    lat_count, lon_count, rows, cols, stencil = sizes
    depth, tile, cells = raw.shape
    pair = 2 * rows
    sides = 1 if lon_count == 2 else 2
    group = tile + sides * tile
    places = BANDS * group
    picks = tile * stencil
    pitch = depth + PAD
    total_cols = cols * lon_count
    lat_rows = (2 * REACH + 1) * rows
    z = lax.axis_index("lat")
    x = lax.axis_index("lon")
    east = lax.rem(x + 1, lon_count)
    west = lax.rem(x + lon_count - 1, lon_count)
    out_side = (east, west)[:sides]
    back = (0,) if sides == 1 else (1, 0)
    last = lat_count - 1
    polar = (z == 0) | (z == last)
    inland = jnp.logical_not(polar)
    poles = ((0, 1), (last, -1))
    kinds = (0, 1)

    def there(offset):
        return (z + offset >= 0) & (z + offset < lat_count)

    def slot(band, kind, side=None):
        first = (band + REACH) * group + kind * pair
        if side is not None:
            first += tile * (1 + side)
        return pl.ds(first, pair)

    def when(condition, act):
        pl.when(condition)(act)

    def loads():
        return (
            pltpu.make_async_copy(own_hbm, raw, load_sem.at[0]),
            pltpu.make_async_copy(forcing_hbm, forcing, load_sem.at[1]),
            pltpu.make_async_copy(weights_hbm, weights, load_sem.at[2]),
            pltpu.make_async_copy(rows_hbm, rows_ref, load_sem.at[3]),
            pltpu.make_async_copy(cols_hbm, cols_ref, load_sem.at[4]),
        )

    barrier = pltpu.get_barrier_semaphore()
    for side in out_side:
        pl.semaphore_signal(barrier, inc=1, device_id={"lon": side}, device_id_type=MESH)
    for step in STEPS:
        @pl.when(there(step))
        def _():
            pl.semaphore_signal(barrier, inc=1, device_id={"lat": z + step}, device_id_type=MESH)
    for copy in loads():
        copy.start()

    def zf(d, hop, kind):
        band = -STEPS[d] * hop
        return pltpu.make_async_remote_copy(
            src_ref=ext.at[:, slot(band, kind), :],
            dst_ref=ext.at[:, slot(band - STEPS[d], kind), :],
            send_sem=zf_send.at[d, hop, kind],
            recv_sem=zf_recv.at[d, hop, kind],
            device_id={"lat": z + STEPS[d]},
            device_id_type=MESH,
        )

    def xf(band, kind, side):
        return pltpu.make_async_remote_copy(
            src_ref=ext.at[:, slot(band, kind), :],
            dst_ref=ext.at[:, slot(band, kind, back[side]), :],
            send_sem=xf_send.at[band + REACH, kind, side],
            recv_sem=xf_recv.at[band + REACH, kind, back[side]],
            device_id={"lon": out_side[side]},
            device_id_type=MESH,
        )

    def xf_in(band, kind, side):
        return pltpu.make_async_remote_copy(
            src_ref=ext.at[:, slot(band, kind), :],
            dst_ref=ext.at[:, slot(band, kind, side), :],
            send_sem=xf_send.at[band + REACH, kind, side],
            recv_sem=xf_recv.at[band + REACH, kind, side],
            device_id={"lon": out_side[side]},
            device_id_type=MESH,
        )

    def ax(band, kind, side, arrive=False):
        land = side if arrive else back[side]
        return pltpu.make_async_remote_copy(
            src_ref=ax_out.at[band + REACH, side, kind],
            dst_ref=ax_in.at[band + REACH, land, kind],
            send_sem=ax_send.at[band + REACH, kind, side],
            recv_sem=ax_recv.at[band + REACH, kind, land],
            device_id={"lon": out_side[side]},
            device_id_type=MESH,
        )

    def az(d, near, kind):
        return pltpu.make_async_remote_copy(
            src_ref=(near_out if near else far_out).at[d, kind],
            dst_ref=(near_in if near else far_in).at[d, kind],
            send_sem=az_send.at[d, near, kind],
            recv_sem=az_recv.at[d, near, kind],
            device_id={"lat": z + STEPS[d]},
            device_id_type=MESH,
        )

    def fwd(pole, step, i, side):
        return pltpu.make_async_remote_copy(
            src_ref=ext.at[:, slot(i * step, 0, side), :],
            dst_ref=ext.at[:, slot((i + 1) * step, 0, side), :],
            send_sem=fwd_send.at[i, side],
            recv_sem=fwd_recv.at[i, side],
            device_id={"lat": pole},
            device_id_type=MESH,
        )

    def lend(pole, step, i, side):
        return pltpu.make_async_remote_copy(
            src_ref=ax_out.at[(i + 1) * step + REACH, side, 0],
            dst_ref=lent.at[i, side],
            send_sem=lend_send.at[i, side],
            recv_sem=lend_recv.at[i, side],
            device_id={"lat": pole + step},
            device_id_type=MESH,
        )

    def x_start(make, band, kind):
        for side in range(sides):
            make(band, kind, side).start()

    span = tile * 8
    to = lax.broadcasted_iota(jnp.int32, (span, span), 0)
    come = lax.broadcasted_iota(jnp.int32, (span, span), 1)

    def column_of(place):
        position = (place % tile) // rows
        return jnp.where(position < 2, position * (cols - 1), position - 1)

    def shuffle(a, b):
        same = (a // tile == b // tile) & (b % tile == (a % rows) * cols + column_of(a))
        return jnp.where(same, 1.0, 0.0).astype(BF16)

    order = shuffle(to, come)
    own = pl.ds(REACH * group, tile)
    loads()[0].wait()
    for i in range(depth // 8):
        block = raw[pl.ds(i * 8, 8)].reshape(span, cells)
        block = jnp.dot(order, block, preferred_element_type=F32).astype(BF16)
        ext[pl.ds(i * 8, 8), own, :] = block.reshape(8, tile, cells)

    greeted = sides + jnp.where(there(1), 1, 0) + jnp.where(there(-1), 1, 0)
    pl.semaphore_wait(barrier, greeted)

    for kind in kinds:
        for d in range(2):
            when(there(STEPS[d]), lambda: zf(d, 0, kind).start())
        if kind == 0:
            x_start(xf, 0, 0)
        else:
            when(polar, lambda: x_start(xf, 0, 1))

    blank = jnp.zeros((depth, tile, cells), BF16)
    for band in range(-REACH, REACH + 1):
        @pl.when(jnp.logical_not(there(band)))
        def _():
            for part in range(group // tile):
                ext[:, pl.ds((band + REACH) * group + part * tile, tile), :] = blank

        @pl.when(there(band) & inland)
        def _():
            for side in range(sides):
                ext[:, slot(band, 1, side), :] = jnp.zeros((depth, pair, cells), BF16)

    lane = lax.broadcasted_iota(jnp.int32, (1, places), 1)
    within = lane % group
    half = within % tile
    position = HALO + jnp.where(half // rows < 2, (half // rows) * (cols - 1), half // rows - 1)
    area = within // tile
    position = position + jnp.where(area == 1, cols, jnp.where(area == 2, -cols, 0))
    position = (position + total_cols) % total_cols
    code = position * lat_rows + (lane // group) * rows + half % rows

    for copy in loads()[3:]:
        copy.wait()

    def select(t, carry):
        i, j = t // cols, t % cols
        for k in range(stencil):
            row = rows_ref[i, j, k] - z * rows + REACH * rows
            col = cols_ref[i, j, k] - x * cols + HALO
            col = col + jnp.where(col < 0, total_cols, 0)
            col = col - jnp.where(col >= total_cols, total_cols, 0)
            gather[pl.ds(t * stencil + k, 1), :] = jnp.where(
                code == col * lat_rows + row, 1.0, 0.0
            )
        return carry

    lax.fori_loop(0, tile, select, 0, unroll=8)
    chosen = gather[...]
    scatter = chosen.T.astype(BF16)

    loads()[1].wait()

    def turn(d, carry):
        turned[pl.ds(d, tile, stride=pitch), :] = forcing[d].astype(F32)
        return carry

    lax.fori_loop(0, depth, turn, 0, unroll=8)
    loads()[2].wait()

    def contribute(t, carry):
        block = weights[pl.ds(t * stencil, stencil)].reshape(stencil * cells, cells)
        here = turned[pl.ds(pl.multiple_of(t * pitch, 8), depth), :].astype(BF16)
        part = lax.dot_general(
            here, block, (((1,), (1,)), ((), ())), preferred_element_type=F32
        )
        for k in range(stencil):
            picked[pl.ds(t * stencil + k, depth, stride=picks + PAD), :] = part[
                :, k * cells : (k + 1) * cells
            ]
        return carry

    lax.fori_loop(0, tile, contribute, 0, unroll=8)

    def add_up(i, carry):
        pieces = []
        for e in range(2):
            first = pl.multiple_of((i * 2 + e) * (picks + PAD), 8)
            pieces.append(picked[pl.ds(first, picks), :].astype(BF16))
        summed = jnp.dot(
            scatter, jnp.concatenate(pieces, axis=1), preferred_element_type=F32
        )
        for e in range(2):
            d = i * 2 + e
            value = summed[:, e * cells : (e + 1) * cells]
            for band in range(BANDS):
                first = band * group
                spread[d, pl.ds(band * tile, tile), :] = value[first : first + tile]
                for side in range(sides):
                    first += tile
                    for kind in kinds:
                        ax_out[band, side, kind, d] = value[
                            first + kind * pair : first + (kind + 1) * pair
                        ].astype(BF16)
        return carry

    lax.fori_loop(0, depth // 2, add_up, 0, unroll=8)

    def total(band, kind):
        return spread.at[:, pl.ds((band + REACH) * tile + kind * pair, pair), :]

    def take(band, kind):
        for side in range(sides):
            ax(band, kind, side, True).wait_recv()
            total(band, kind)[...] += ax_in[band + REACH, side, kind].astype(F32)

    def send_far(d, kind):
        far_out[d, kind] = total(2 * STEPS[d], kind)[...].astype(BF16)
        az(d, 0, kind).start()

    def send_near(d, kind):
        @pl.when(there(-STEPS[d]))
        def _():
            az(d, 0, kind).wait_recv()
            total(STEPS[d], kind)[...] += far_in[d, kind].astype(F32)

        near_out[d, kind] = total(STEPS[d], kind)[...].astype(BF16)
        az(d, 1, kind).start()

    def borrow(pole, step, i):
        for side in range(sides):
            lend(pole, step, i, side).wait_recv()
            mine = ax_out.at[i * step + REACH, side, 0]
            mine[...] = (mine[...].astype(F32) + lent[i, side].astype(F32)).astype(BF16)
        x_start(ax, i * step, 0)

    for pole, step in poles:
        @pl.when(z == pole)
        def _():
            x_start(ax, 2 * step, 1)
            for side in range(sides):
                lend(pole, step, 1, side).start()
    for d in range(2):
        when(there(2 * STEPS[d]) & inland, lambda: x_start(ax, 2 * STEPS[d], 0))
    for pole, step in poles:
        when(z == pole, lambda: send_far(STEPS.index(step), 0))
    for d in range(2):
        @pl.when(there(-STEPS[d]))
        def _():
            zf(d, 0, 0).wait_recv()
            when(there(STEPS[d]), lambda: zf(d, 1, 0).start())
    for pole, step in poles:
        @pl.when(z == pole + step)
        def _():
            for side in range(sides):
                xf_in(0, 0, side).wait_recv()
            for side in range(sides):
                fwd(pole, step, 0, side).start()
            x_start(xf, step, 0)
            x_start(ax, -step, 0)
    inner = (z > 1) & (z < last - 1)

    @pl.when(inner)
    def _():
        for step in STEPS:
            x_start(ax, step, 0)
            x_start(xf, step, 0)

    for d in range(2):
        when(there(2 * STEPS[d]) & inland, lambda: send_far(d, 1))
    for d in range(2):
        @pl.when(there(-STEPS[d]))
        def _():
            zf(d, 0, 1).wait_recv()
            when(there(STEPS[d]), lambda: zf(d, 1, 1).start())
    for pole, step in poles:
        @pl.when(z == pole)
        def _():
            x_start(xf, step, 1)
            x_start(ax, step, 1)
            take(2 * step, 1)
            send_far(STEPS.index(step), 1)
            for side in range(sides):
                lend(pole, step, 0, side).start()
            send_near(STEPS.index(step), 0)
    for d in range(2):
        @pl.when(there(2 * STEPS[d]) & inland)
        def _():
            take(2 * STEPS[d], 0)
            send_far(d, 0)
    for pole, step in poles:
        @pl.when(z == pole + step)
        def _():
            borrow(pole, step, 1)
            x_start(xf, -step, 0)
            for side in range(sides):
                xf_in(step, 0, side).wait_recv()
            for side in range(sides):
                fwd(pole, step, 1, side).start()
    for d in range(2):
        @pl.when(there(-2 * STEPS[d]))
        def _():
            zf(d, 1, 0).wait_recv()
            when(inland, lambda: x_start(xf, -2 * STEPS[d], 0))
    for d in range(2):
        @pl.when(there(-2 * STEPS[d]))
        def _():
            zf(d, 1, 1).wait_recv()
            when(polar, lambda: x_start(xf, -2 * STEPS[d], 1))
    when(inner, lambda: x_start(ax, 0, 0))
    for pole, step in poles:
        @pl.when(z == pole)
        def _():
            x_start(ax, 0, 0)
            x_start(ax, 0, 1)
    for pole, step in poles:
        @pl.when(z == pole)
        def _():
            take(step, 1)
            send_near(STEPS.index(step), 1)

        @pl.when(z == pole + step)
        def _():
            send_near(STEPS.index(step), 1)
            take(-step, 0)
            send_near(STEPS.index(-step), 0)
            send_near(STEPS.index(-step), 1)
            take(step, 0)
            send_near(STEPS.index(step), 0)
            borrow(pole, step, 0)

    @pl.when(inner)
    def _():
        for d in range(2):
            send_near(d, 1)
        for d in range(2):
            take(STEPS[d], 0)
            send_near(d, 0)

    for pole, step in poles:
        @pl.when(z == pole)
        def _():
            for side in range(sides):
                for kind in kinds:
                    xf_in(0, kind, side).wait_recv()
                for i in range(2):
                    xf_in((i + 1) * step, 1, side).wait_recv()
                    fwd(pole, step, i, side).wait_recv()

        @pl.when(z == pole + step)
        def _():
            for side in range(sides):
                xf_in(-step, 0, side).wait_recv()

    @pl.when(inner)
    def _():
        for band in range(-1, 2):
            for side in range(sides):
                xf_in(band, 0, side).wait_recv()

    for d in range(2):
        @pl.when(there(2 * STEPS[d]) & inland)
        def _():
            for side in range(sides):
                xf_in(2 * STEPS[d], 0, side).wait_recv()

    chosen = gather[...].astype(BF16)

    def collect(i, carry):
        block = jnp.concatenate([ext[i * 2], ext[i * 2 + 1]], axis=1)
        value = jnp.dot(chosen, block, preferred_element_type=F32)
        for e in range(2):
            picked[pl.ds(i * 2 + e, picks, stride=pitch), :] = value[
                :, e * cells : (e + 1) * cells
            ]
        return carry

    lax.fori_loop(0, depth // 2, collect, 0, unroll=8)

    def interpolate(t, carry):
        sources = []
        for k in range(stencil):
            first = pl.multiple_of((t * stencil + k) * pitch, 8)
            sources.append(picked[pl.ds(first, depth), :].astype(BF16))
        block = weights[pl.ds(t * stencil, stencil)].reshape(stencil * cells, cells)
        value = jnp.dot(
            jnp.concatenate(sources, axis=1), block, preferred_element_type=F32
        )
        tangent_ref[t] = value.astype(BF16)
        return carry

    lax.fori_loop(0, tile, interpolate, 0, unroll=8)

    take(0, 0)
    when(polar, lambda: take(0, 1))
    for d in range(2):
        @pl.when(there(-STEPS[d]))
        def _():
            for kind in kinds:
                az(d, 1, kind).wait_recv()
                total(0, kind)[...] += near_in[d, kind].astype(F32)
    order = shuffle(come, to)
    for i in range(depth // 8):
        block = spread[pl.ds(i * 8, 8), pl.ds(REACH * tile, tile), :].astype(BF16)
        block = jnp.dot(order, block.reshape(span, cells), preferred_element_type=F32)
        adjoint_ref[pl.ds(i * 8, 8)] = block.astype(BF16).reshape(8, tile, cells)

    for d in range(2):
        @pl.when(there(STEPS[d]))
        def _():
            for kind in kinds:
                zf(d, 0, kind).wait_send()
                az(d, 1, kind).wait_send()

                @pl.when(there(-STEPS[d]))
                def _():
                    zf(d, 1, kind).wait_send()

                @pl.when(there(2 * STEPS[d]))
                def _():
                    az(d, 0, kind).wait_send()
    for side in range(sides):
        for make in (xf, ax):
            make(0, 0, side).wait_send()
            for band in range(-REACH, REACH + 1):
                if band != 0:
                    when(there(band) & inland, lambda: make(band, 0, side).wait_send())
                when(there(band) & polar, lambda: make(band, 1, side).wait_send())
        for pole, step in poles:
            for i in range(2):
                when(z == pole, lambda: lend(pole, step, i, side).wait_send())
                when(z == pole + step, lambda: fwd(pole, step, i, side).wait_send())


def on_device(perturbation, adjoint_forcing, source_rows, source_cols, cubic_weights):
    fields, levels, rows, cols, cells = perturbation.shape
    stencil = source_rows.shape[2]
    depth = fields * levels
    tile = rows * cols
    picks = tile * stencil
    lat_count = lax.axis_size("lat")
    lon_count = lax.axis_size("lon")
    assert cols == 2 * HALO and rows >= 4 and lat_count >= 4 and lon_count >= 2
    sides = 1 if lon_count == 2 else 2
    places = BANDS * tile * (1 + sides)
    half = (depth, 2 * rows, cells)
    indices = [pltpu.with_memory_space_constraint(a, pltpu.HBM) for a in (source_rows, source_cols)]
    own, forcing, weights = (
        pltpu.with_memory_space_constraint(a, pltpu.HBM)
        for a in (
            perturbation.reshape(depth, tile, cells),
            adjoint_forcing.reshape(depth, tile, cells),
            cubic_weights.reshape(picks, cells, cells),
        )
    )

    vmem = pl.BlockSpec(memory_space=pltpu.VMEM)
    hbm = pl.BlockSpec(memory_space=pltpu.HBM)
    dma = pltpu.SemaphoreType.DMA
    tangent, adjoint = pl.pallas_call(
        functools.partial(exchange, (lat_count, lon_count, rows, cols, stencil)),
        name="exchange",
        out_shape=(
            jax.ShapeDtypeStruct((tile, depth, cells), BF16),
            jax.ShapeDtypeStruct((depth, tile, cells), BF16),
        ),
        in_specs=[hbm] * 5,
        out_specs=(vmem, vmem),
        scratch_shapes=[
            pltpu.SMEM(source_rows.shape, jnp.int32),
            pltpu.SMEM(source_cols.shape, jnp.int32),
            pltpu.VMEM((depth, tile, cells), BF16),
            pltpu.VMEM((depth, tile, cells), BF16),
            pltpu.VMEM((picks, cells, cells), BF16),
            pltpu.VMEM((depth, places, cells), BF16),
            pltpu.VMEM((max(picks, depth) * (max(picks, depth) + PAD), cells), F32),
            pltpu.VMEM((tile * (depth + PAD), cells), F32),
            pltpu.VMEM((depth, BANDS * tile, cells), F32),
            pltpu.VMEM((picks, places), F32),
            pltpu.VMEM((BANDS, sides, 2) + half, BF16),
            pltpu.VMEM((BANDS, sides, 2) + half, BF16),
            pltpu.VMEM((2, 2) + half, BF16),
            pltpu.VMEM((2, 2) + half, BF16),
            pltpu.VMEM((2, 2) + half, BF16),
            pltpu.VMEM((2, 2) + half, BF16),
            pltpu.VMEM((2, sides) + half, BF16),
            dma((5,)),
            dma((2, 2, 2)),
            dma((2, 2, 2)),
            dma((BANDS, 2, sides)),
            dma((BANDS, 2, sides)),
            dma((BANDS, 2, sides)),
            dma((BANDS, 2, sides)),
            dma((2, 2, 2)),
            dma((2, 2, 2)),
            dma((2, sides)),
            dma((2, sides)),
            dma((2, sides)),
            dma((2, sides)),
        ],
        compiler_params=pltpu.CompilerParams(
            collective_id=0, has_side_effects=True, vmem_limit_bytes=24 * 1024 * 1024
        ),
    )(*indices, own, forcing, weights)

    tangent_out = tangent.reshape(rows, cols, fields, levels, cells).transpose(2, 3, 0, 1, 4)
    adjoint_out = adjoint.reshape(fields, levels, rows, cols, cells)
    return (tangent_out, adjoint_out)


def solution(mesh):
    placed = (
        P("member", "lev", "lat", "lon", None),
        P("member", "lev", "lat", "lon", None),
        P("lat", "lon", None),
        P("lat", "lon", None),
        P("lat", "lon", None, None, None),
    )
    return jax.shard_map(
        on_device,
        mesh=mesh,
        in_specs=placed,
        out_specs=(P("member", "lev", "lat", "lon", None), P("member", "lev", "lat", "lon", None)),
        check_vma=False,
    )
```
